32 devices in a mesh: lon: 4 (over z), lat: 8 (over y, x, core).
Axes of the slice: x: 2, y: 2, z: 4, core: 2. Of those that a mesh axis runs over, the one named last changes fastest.
Arguments:
- fields: float32 [4, 8, 512, 3600], P(None, None, 'lat', 'lon'), may hold values from -6 to 6
- thickness: float32 [8], replicated, may hold values from 5 to 250
- cutoff: int32 [256], replicated, may hold values from 2 to 1800
- barotropic: float32 [3, 512, 3600], P(None, 'lat', 'lon'), may hold values from -6 to 6
- land_sea: int32 [512, 3600], P('lat', 'lon'), may hold values 0 or 1
Outputs:
- filtered_tracers: float32 [2, 8, 512, 3600], P(None, None, 'lat', 'lon')
- velocity: float32 [2, 8, 512, 3600], P(None, None, 'lat', 'lon')
- sea_level: float32 [512, 3600], P('lat', 'lon')
The draws below stay inside these ranges and needn't reach their ends.
Inputs may be any that keep to these rules, and one draw needn't show every extreme that they name: `cutoff`: each filtered row's highest kept wavenumber.
All inputs are finite; a program needn't handle non-finite values. No bound on the sum of `land_sea` on one device may be relied on, other than what follows from the above.
Results may differ from the reference program's by a relative error of at most 0.0003.
Values sent between devices are 32-bit elements; how exact they have to be, the bound alone decides.
A program may use at most 128 MiB of HBM per device.

```python
import math
import jax
import jax.numpy as jnp
from jax import lax

NLON = 3600
LEV = 8
SUB = 20
NLAT = 512
NPOLE = 128


def touch_ends(drawn, own_key, smallest, largest):
    extent = drawn.shape
    index_at = [jax.random.randint(jax.random.fold_in(own_key, axis), (), 0, extent[axis]) for axis in range(len(extent))]
    drawn = drawn.at[tuple(index_at)].set(smallest)
    longest = extent.index(max(extent))
    index_at[longest] = (index_at[longest] + 1) % extent[longest]
    return drawn.at[tuple(index_at)].set(largest)


def shard_levels(own_key, dims, split, least, top_value):
    def one(dim, shards_of):
        heights = jax.random.uniform(jax.random.fold_in(jax.random.fold_in(own_key, 6), dim), (shards_of,), jnp.float32, least / len(split), top_value / len(split))
        return jnp.repeat(jnp.exp(heights), dims[dim] // shards_of).reshape((-1,) + (1,) * (len(dims) - dim - 1))

    level = one(*split[0])
    for cut in split[1:]:
        level = level * one(*cut)
    return level


def gaussian(rng, dims, scale, most, shards=(), kind=jnp.bfloat16):
    drawn = scale * jax.random.normal(rng, dims, jnp.float32)
    if shards:
        drawn = drawn * shard_levels(rng, dims, shards, -0.22, 0.18)
    return jnp.clip(drawn, -most, most).astype(kind)


def setup_inputs(seed: int = 0) -> dict:
    arg_keys = jax.random.split(jax.random.key(seed), 6)
    fields = gaussian(arg_keys[0], (4, LEV, NLAT, NLON), 1.0, 6.0, ((2, 8), (3, 4)), jnp.float32)
    thickness = jnp.clip(jnp.exp(jax.random.uniform(arg_keys[1], (LEV,), jnp.float32, math.log(5.0), math.log(250.0))), 5.0, 250.0)
    cutoff = touch_ends(jax.random.randint(arg_keys[2], (2 * NPOLE,), 2, NLON // 2 + 1), jax.random.fold_in(arg_keys[2], 1), 2, (NLON // 2 + 1) - 1).astype(jnp.int32)
    barotropic = gaussian(arg_keys[3], (3, NLAT, NLON), 1.0, 6.0, ((1, 8), (2, 4)), jnp.float32)
    land_sea = touch_ends((jax.random.randint(arg_keys[4], (NLAT, NLON), 0, 5) < 4).astype(jnp.int32), jax.random.fold_in(arg_keys[4], 1), 0, 1)
    return {"fields": fields, "thickness": thickness, "cutoff": cutoff, "barotropic": barotropic, "land_sea": land_sea}


wave_coef = 0.65


def polar_filter(values, row_cuts):
    circle_len = values.shape[-1]
    spectrum = jnp.fft.rfft(values, axis=-1)
    wavenumber = jnp.arange(circle_len // 2 + 1)
    kept_mask = wavenumber[None, :] <= row_cuts[:, None]
    return jnp.fft.irfft(spectrum * kept_mask, n=circle_len, axis=-1).astype(values.dtype)


def reference(fields, thickness, cutoff, barotropic, land_sea):
    total_rows = fields.shape[2]
    pole_rows = cutoff.shape[0] // 2
    north_rows = polar_filter(fields[:, :, :pole_rows], cutoff[:pole_rows])
    south_rows = polar_filter(fields[:, :, total_rows - pole_rows:], cutoff[pole_rows:])
    filtered = jnp.concatenate([north_rows, fields[:, :, pole_rows:total_rows - pole_rows], south_rows], axis=2)
    ocean_cell = land_sea.astype(fields.dtype)
    row_number = jnp.arange(total_rows)
    east_open = ocean_cell * jnp.roll(ocean_cell, -1, 1)
    north_open = ocean_cell * jnp.roll(ocean_cell, -1, 0) * (row_number != total_rows - 1).astype(fields.dtype)[:, None]
    surface = barotropic[0]
    eastward = barotropic[1] * east_open
    northward = barotropic[2] * north_open
    for subcycle in range(SUB):
        divergence = eastward - jnp.roll(eastward, 1, 1) + northward - jnp.roll(northward, 1, 0)
        surface = surface - wave_coef * ocean_cell * divergence
        eastward = east_open * (eastward - wave_coef * (jnp.roll(surface, -1, 1) - surface))
        northward = north_open * (northward - wave_coef * (jnp.roll(surface, -1, 0) - surface))
    weights = thickness / jnp.sum(thickness)
    currents = filtered[2:]
    column = jnp.einsum("k,ckij->cij", weights, currents, precision=lax.Precision.HIGHEST)
    velocity = jnp.stack([east_open, north_open])[:, None] * (currents - column[:, None] + jnp.stack([eastward, northward])[:, None])
    return filtered[:2], velocity, surface
```

```python
import functools
import math

import jax
import jax.numpy as jnp
import numpy as np
from jax import lax
from jax.experimental import pallas as pl
from jax.experimental.pallas import tpu as pltpu
from jax.sharding import PartitionSpec as P

SUB = 20
HALO = -(-(SUB + 2) // 8) * 8
wave_coef = 0.65
RESIDUAL = 3e-8


def two_part(table):
    high = table.astype(jnp.bfloat16)
    low = (table - high.astype(np.float64)).astype(jnp.bfloat16)
    return high, low


def cosecant(circle, cols, shift):
    gap = (np.arange(cols)[None, :] + shift - np.arange(cols)[:, None]).astype(np.float64)
    sine = np.sin(np.pi * gap / circle)
    near = gap == 0
    return np.where(near, 0.0, 1.0 / np.where(near, 1.0, sine)) / circle


def cross_factors(block):
    rest = block.copy()
    left, right = [], []
    while True:
        spot = np.unravel_index(np.argmax(np.abs(rest)), rest.shape)
        pivot = rest[spot]
        if abs(pivot) < RESIDUAL:
            break
        column = rest[:, spot[1]] / math.sqrt(abs(pivot))
        row = rest[spot[0]] * (math.copysign(1.0, pivot) / math.sqrt(abs(pivot)))
        left.append(column)
        right.append(row)
        rest = rest - column[:, None] * row[None, :]
    pad = -len(left) % 8
    zero = [np.zeros(block.shape[0])] * pad
    return np.stack(left + zero), np.stack(right + zero)


@functools.lru_cache(maxsize=None)
def tables(circle, cols):
    devices = circle // cols
    pairs = [cross_factors(cosecant(circle, cols, cols * o)) for o in range(1, devices)]
    ranks = tuple(p[0].shape[0] for p in pairs)
    send = np.concatenate([p[0] for p in pairs])
    take = np.concatenate([p[1] for p in pairs])
    return ranks, two_part(cosecant(circle, cols, 0)), two_part(send), two_part(take)


def split(value):
    high = value.astype(jnp.bfloat16)
    low = (value - high.astype(jnp.float32)).astype(jnp.bfloat16)
    return high, low


def product(a, b, dims):
    def dot(p, q):
        return lax.dot_general(p, q, (dims, ((), ())), preferred_element_type=jnp.float32)

    return dot(a[0], b[0]) + (dot(a[1], b[0]) + dot(a[0], b[1]))


def turned(x, cos, sin):
    levels, rows, cols = x.shape
    both = jnp.concatenate([x * cos[None], x * sin[None]], axis=0)
    return split(both.reshape(2 * levels * rows, cols))


def moment_kernel(ranks, x_ref, cos_ref, sin_ref, high_ref, low_ref, sign_ref, *out_refs):
    wave = turned(x_ref[0], cos_ref[...], sin_ref[...])
    moments = product((high_ref[...], low_ref[...]), wave, ((1,), (1,)))
    moments = moments * sign_ref[:, 0:1]
    start = 0
    for rank, out_ref in zip(ranks, out_refs):
        out_ref[...] = moments[start : start + rank]
        start += rank


def filtered_block(n_far, refs):
    x_ref, cos_ref, sin_ref, diag_ref, near_high, near_low, far_high, far_low = refs[:8]
    x = x_ref[0]
    levels, rows, cols = x.shape
    cos, sin = cos_ref[...], sin_ref[...]
    total = product(turned(x, cos, sin), (near_high[...], near_low[...]), ((1,), (0,)))
    far = jnp.concatenate([r[...] for r in refs[8 : 8 + n_far]], axis=0)
    total = total + product(split(far.T), (far_high[...], far_low[...]), ((1,), (0,)))
    total = total.reshape(2, levels, rows, cols)
    return sin[None] * total[0] - cos[None] * total[1] + diag_ref[:, 0:1][None] * x


def tracer_kernel(n_far, *refs):
    refs[-1][0] = filtered_block(n_far, refs)


def velocity_kernel(n_far, *refs):
    weight_ref, open_ref, flow_ref, out_ref = refs[8 + n_far :]
    value = filtered_block(n_far, refs)
    column = value[0] * weight_ref[0]
    for k in range(1, value.shape[0]):
        column = column + value[k] * weight_ref[k]
    out_ref[0] = open_ref[0][None] * (value - column[None] + flow_ref[0][None])


def subcycle_kernel(rows, cols, pad_ref, level_ref, open_ref, flow_ref, state, opens):
    high, wide = pad_ref.shape[1:]
    ocean = pad_ref[3]
    opens[0] = ocean * wave_coef
    opens[1] = ocean * pltpu.roll(ocean, wide - 1, 1)
    opens[2] = ocean * pltpu.roll(ocean, high - 1, 0)
    state[0] = pad_ref[0]
    state[1] = pad_ref[1] * opens[1]
    state[2] = pad_ref[2] * opens[2]

    def step(i, carry):
        east, north = state[1], state[2]
        div = east - pltpu.roll(east, 1, 1) + north - pltpu.roll(north, 1, 0)
        surface = state[0] - opens[0] * div
        state[0] = surface
        state[1] = opens[1] * (
            east - wave_coef * (pltpu.roll(surface, wide - 1, 1) - surface)
        )
        state[2] = opens[2] * (
            north - wave_coef * (pltpu.roll(surface, high - 1, 0) - surface)
        )
        return carry

    lax.fori_loop(0, SUB, step, 0)
    level_ref[...] = state[0, :rows, :cols]
    open_ref[...] = opens[1:, :rows, :cols]
    flow_ref[...] = state[1:, :rows, :cols]


def shifted(value, axis, offset, ring):
    count = lax.axis_size(axis)
    pairs = [(i, (i + offset) % count) for i in range(count) if ring or 0 <= i + offset < count]
    return lax.ppermute(value, axis, pairs)


def barotropic_steps(barotropic, land_sea):
    rows, cols = land_sea.shape
    own = jnp.concatenate([barotropic, land_sea.astype(jnp.float32)[None]])
    west = shifted(own[:, :, cols - HALO :], "lon", 1, True)
    east = shifted(own[:, :, :HALO], "lon", -1, True)
    gap = -(cols + 2 * HALO) % 128
    wide = jnp.concatenate([own, east, jnp.zeros((4, rows, gap), jnp.float32), west], axis=2)
    south = shifted(wide[:, rows - HALO :], "lat", 1, False)
    north = shifted(wide[:, :HALO], "lat", -1, False)
    padded = jnp.concatenate([wide, north, south], axis=1)
    shape = padded.shape[1:]
    pair = jax.ShapeDtypeStruct((2, rows, cols), jnp.float32)
    return pl.pallas_call(
        functools.partial(subcycle_kernel, rows, cols),
        out_shape=(jax.ShapeDtypeStruct((rows, cols), jnp.float32), pair, pair),
        scratch_shapes=[pltpu.VMEM((3,) + shape, jnp.float32)] * 2,
        cost_estimate=pl.CostEstimate(
            flops=SUB * 100 * shape[0] * shape[1], bytes_accessed=0, transcendentals=0
        ),
        name="subcycles",
    )(padded)


def body(fields, thickness, cutoff, barotropic, land_sea):
    lon_count, lat_count = lax.axis_size("lon"), lax.axis_size("lat")
    lat_index, lon_index = lax.axis_index("lat"), lax.axis_index("lon")
    components, levels, rows, cols = fields.shape
    circle, total_rows = cols * lon_count, rows * lat_count
    ranks, near, send, take = tables(circle, cols)
    n_far = len(ranks)

    pole_rows = cutoff.shape[0] // 2
    row_ids = lat_index * rows + lax.iota(jnp.int32, rows)
    slots = jnp.where(row_ids < pole_rows, row_ids, row_ids - (total_rows - 2 * pole_rows))
    polar = (row_ids < pole_rows) | (row_ids >= total_rows - pole_rows)
    match = slots[:, None] == lax.broadcasted_iota(jnp.int32, (1, 2 * pole_rows), 1)
    cuts = jnp.sum(jnp.where(match, cutoff[None, :], 0), axis=1)
    cut_rows = polar & (2 * cuts < circle)
    odd = jnp.where(cut_rows, 2 * cuts + 1, 0)
    place = lon_index * cols + lax.iota(jnp.int32, cols)
    angle = ((odd[:, None] * place[None, :]) % (2 * circle)).astype(jnp.float32) * (
        math.pi / circle
    )
    cos = jnp.where(cut_rows[:, None], jnp.cos(angle), 0.0)
    sin = jnp.where(cut_rows[:, None], jnp.sin(angle), 0.0)
    diag = jnp.where(cut_rows, odd.astype(jnp.float32) / circle, 1.0)
    diag = jnp.broadcast_to(diag[:, None], (rows, 128))
    offsets = np.repeat(np.arange(1, lon_count), ranks)
    sign = jnp.where(lon_index + offsets >= lon_count, -1.0, 1.0).astype(jnp.float32)
    sign = jnp.broadcast_to(sign[:, None], (sum(ranks), 128))

    take_rows = 32 if rows % 32 == 0 else rows
    steps = rows // take_rows
    items = 2 * levels * take_rows
    part = components // 2

    def whole(array):
        return pl.BlockSpec(array.shape, lambda f, h: (0,) * array.ndim)

    def field_spec(first):
        return pl.BlockSpec((1, levels, take_rows, cols), lambda f, h: (f + first, 0, h, 0))

    row_spec = pl.BlockSpec((take_rows, cols), lambda f, h: (h, 0))
    diag_spec = pl.BlockSpec((take_rows, 128), lambda f, h: (h, 0))
    pair_spec = pl.BlockSpec((1, take_rows, cols), lambda f, h: (f, h, 0))

    def moment_specs(first):
        return [pl.BlockSpec((r, items), lambda f, h: (0, (f + first) * steps + h)) for r in ranks]

    moments = pl.pallas_call(
        functools.partial(moment_kernel, ranks),
        grid=(components, steps),
        in_specs=[field_spec(0), row_spec, row_spec, whole(send[0]), whole(send[1]), whole(sign)],
        out_specs=moment_specs(0),
        out_shape=[
            jax.ShapeDtypeStruct((r, components * steps * items), jnp.float32) for r in ranks
        ],
        cost_estimate=pl.CostEstimate(
            flops=20 * fields.size * 64, bytes_accessed=4 * fields.size, transcendentals=0
        ),
        name="moments",
    )(fields, cos, sin, send[0], send[1], sign)
    far = [shifted(m, "lon", o + 1, True) for o, m in enumerate(moments)]

    sea_level, opens, flows = barotropic_steps(barotropic, land_sea)
    weights = thickness / jnp.sum(thickness)

    def apply(kernel, first, specs, args, name):
        return pl.pallas_call(
            functools.partial(kernel, n_far),
            grid=(part, steps),
            in_specs=[field_spec(first), row_spec, row_spec, diag_spec]
            + [whole(t) for t in near + take]
            + moment_specs(first)
            + specs,
            out_specs=field_spec(0),
            out_shape=jax.ShapeDtypeStruct((part,) + fields.shape[1:], jnp.float32),
            cost_estimate=pl.CostEstimate(
                flops=12 * part * levels * rows * cols * cols,
                bytes_accessed=4 * fields.size,
                transcendentals=0,
            ),
            name=name,
        )(fields, cos, sin, diag, *near, *take, *far, *args)

    tracers = apply(tracer_kernel, 0, [], [], "tracers")
    smem = pl.BlockSpec(memory_space=pltpu.SMEM)
    velocity = apply(
        velocity_kernel, part, [smem, pair_spec, pair_spec], [weights, opens, flows], "velocity"
    )
    return tracers, velocity, sea_level


def solution(mesh):
    return jax.shard_map(
        body,
        mesh=mesh,
        in_specs=(P(None, None, "lat", "lon"), P(), P(), P(None, "lat", "lon"), P("lat", "lon")),
        out_specs=(P(None, None, "lat", "lon"), P(None, None, "lat", "lon"), P("lat", "lon")),
        check_vma=False,
    )
```

```python
import functools
import math

import jax
import jax.numpy as jnp
import numpy as np
from jax import lax
from jax.experimental import pallas as pl
from jax.experimental.pallas import tpu as pltpu
from jax.sharding import PartitionSpec as P

SUB = 20
HALO = -(-(SUB + 2) // 8) * 8
wave_coef = 0.65
RESIDUAL = 3e-8


def two_part(table):
    high = table.astype(jnp.bfloat16)
    low = (table - high.astype(np.float64)).astype(jnp.bfloat16)
    return high, low


def cosecant(circle, cols, shift):
    gap = (np.arange(cols)[None, :] + shift - np.arange(cols)[:, None]).astype(np.float64)
    sine = np.sin(np.pi * gap / circle)
    near = gap == 0
    return np.where(near, 0.0, 1.0 / np.where(near, 1.0, sine)) / circle


def cross_factors(block):
    rest = block.copy()
    left, right = [], []
    while True:
        spot = np.unravel_index(np.argmax(np.abs(rest)), rest.shape)
        pivot = rest[spot]
        if abs(pivot) < RESIDUAL:
            break
        column = rest[:, spot[1]] / math.sqrt(abs(pivot))
        row = rest[spot[0]] * (math.copysign(1.0, pivot) / math.sqrt(abs(pivot)))
        left.append(column)
        right.append(row)
        rest = rest - column[:, None] * row[None, :]
    pad = -len(left) % 8
    rows, cols = block.shape
    return np.stack(left + [np.zeros(rows)] * pad), np.stack(right + [np.zeros(cols)] * pad)


@functools.lru_cache(maxsize=None)
def tables(circle, cols):
    devices = circle // cols
    cut = -(-cols // 512) * 256
    near = cosecant(circle, cols, 0)
    pairs = [cross_factors(cosecant(circle, cols, cols * o)) for o in range(1, devices)]
    for source, target in ((slice(0, cut), slice(cut, cols)), (slice(cut, cols), slice(0, cut))):
        part = cross_factors(near[source, target])
        whole = [np.zeros((part[0].shape[0], cols)) for _ in range(2)]
        whole[0][:, source], whole[1][:, target] = part
        pairs.append(tuple(whole))
    ranks = tuple(p[0].shape[0] for p in pairs)
    ranks = ranks[: devices - 1] + (sum(ranks[devices - 1 :]),)
    send = two_part(np.concatenate([p[0] for p in pairs]).T)
    width = -(-sum(ranks) // 128) * 128
    room = ((0, 0), (0, width - sum(ranks)))
    send = np.concatenate([np.pad(part, room) for part in send], axis=1)
    take = two_part(np.concatenate([p[1] for p in pairs]))
    take = np.concatenate([take[0], take[0], take[1]])
    side = max(cut, cols - cut)
    return cut, ranks, two_part(near[:side, :side]), send, take


def split(value):
    high = value.astype(jnp.bfloat16)
    low = (value - high.astype(jnp.float32)).astype(jnp.bfloat16)
    return high, low


def dot(a, b):
    return lax.dot_general(a, b, (((1,), (0,)), ((), ())), preferred_element_type=jnp.float32)


def turned(x, cos, sin):
    levels, rows, cols = x.shape
    both = jnp.concatenate([x * cos[None], x * sin[None]], axis=0)
    return split(both.reshape(2 * levels * rows, cols))


def moment_kernel(ranks, x_ref, cos_ref, sin_ref, send_ref, *out_refs):
    cols = x_ref.shape[-1]
    high, low = turned(x_ref[0], cos_ref[:, :cols], sin_ref[...])
    width = send_ref.shape[1] // 2
    both = dot(high, send_ref[...])
    moments = both[:, :width] + (both[:, width:] + dot(low, send_ref[:, :width]))
    moments = moments.T
    count, place = lax.axis_size("lon"), lax.axis_index("lon")
    start = 0
    for offset, (rank, out_ref) in enumerate(zip(ranks, out_refs), 1):
        group = moments[start : start + rank]
        if offset < count:
            group = group * jnp.where(place + offset >= count, -1.0, 1.0)
        out_ref[...] = group
        start += rank


def filtered_block(cut, n_far, refs):
    x_ref, cos_ref, sin_ref, near_high, near_low, take_ref = refs[:6]
    x = x_ref[0]
    levels, rows, cols = x.shape
    cos, sin = cos_ref[:, :cols], sin_ref[...]
    diag = cos_ref[:, cols : cols + 1]
    high, low = turned(x, cos, sin)
    far = jnp.concatenate([r[...] for r in refs[6 : 6 + n_far]], axis=0)
    far_high = far.astype(jnp.bfloat16).astype(jnp.float32)
    far = jnp.concatenate([far_high, far - far_high, far_high], axis=0).T.astype(jnp.bfloat16)
    outs = []
    for a, b in ((0, cut), (cut, cols)):
        n = b - a
        k_high, k_low = near_high[:n, :n], near_low[:n, :n]
        part = dot(high[:, a:b], k_high) + (dot(low[:, a:b], k_high) + dot(high[:, a:b], k_low))
        part = (part + dot(far, take_ref[:, a:b])).reshape(2, levels, rows, n)
        outs.append(
            sin[None, :, a:b] * part[0] - cos[None, :, a:b] * part[1] + diag[None] * x[:, :, a:b]
        )
    return outs


def tracer_kernel(cut, n_far, *refs):
    first, second = filtered_block(cut, n_far, refs)
    refs[-1][0, :, :, :cut] = first
    refs[-1][0, :, :, cut:] = second


def velocity_kernel(cut, n_far, *refs):
    thick_ref, open_ref, flow_ref, out_ref = refs[6 + n_far :]
    first, second = filtered_block(cut, n_far, refs)
    cols = out_ref.shape[-1]
    for value, a, b in ((first, 0, cut), (second, cut, cols)):
        column = value[0] * thick_ref[0]
        depth = thick_ref[0]
        for k in range(1, value.shape[0]):
            column = column + value[k] * thick_ref[k]
            depth = depth + thick_ref[k]
        extra = flow_ref[0, :, a:b] - column / jnp.full(column.shape, depth)
        out_ref[0, :, :, a:b] = open_ref[0, :, a:b][None] * (value + extra[None])


def subcycle_kernel(rows, cols, pad_ref, level_ref, open_ref, flow_ref, state, opens):
    high, wide = pad_ref.shape[1:]
    ocean = pad_ref[3]
    opens[0] = ocean * wave_coef
    opens[1] = ocean * pltpu.roll(ocean, wide - 1, 1)
    opens[2] = ocean * pltpu.roll(ocean, high - 1, 0)
    state[0] = pad_ref[0]
    state[1] = pad_ref[1] * opens[1]
    state[2] = pad_ref[2] * opens[2]

    def step(i, carry):
        east, north = state[1], state[2]
        div = east - pltpu.roll(east, 1, 1) + north - pltpu.roll(north, 1, 0)
        surface = state[0] - opens[0] * div
        state[0] = surface
        state[1] = opens[1] * (
            east - wave_coef * (pltpu.roll(surface, wide - 1, 1) - surface)
        )
        state[2] = opens[2] * (
            north - wave_coef * (pltpu.roll(surface, high - 1, 0) - surface)
        )
        return carry

    lax.fori_loop(0, SUB, step, 0)
    level_ref[...] = state[0, :rows, :cols]
    open_ref[...] = opens[1:, :rows, :cols]
    flow_ref[...] = state[1:, :rows, :cols]


def shifted(value, axis, offset, ring):
    count = lax.axis_size(axis)
    pairs = [(i, (i + offset) % count) for i in range(count) if ring or 0 <= i + offset < count]
    return lax.ppermute(value, axis, pairs)


def tall_tile(barotropic, land_sea):
    rows, cols = land_sea.shape
    own = jnp.concatenate([barotropic, land_sea.astype(jnp.float32)[None]])
    west = shifted(own[:, :, cols - HALO :], "lon", 1, True)
    east = shifted(own[:, :, :HALO], "lon", -1, True)
    gap = -(cols + 2 * HALO) % 128
    wide = jnp.concatenate([own, east, jnp.zeros((4, rows, gap), jnp.float32), west], axis=2)
    last, first = wide[:, rows - HALO :], wide[:, :HALO]
    south = shifted(last, "lat", 1, False)
    north = shifted(first, "lat", -1, False)
    return (last, first), jnp.concatenate([wide, north, south], axis=1)


def barotropic_steps(padded, rows, cols):
    shape = padded.shape[1:]
    pair = jax.ShapeDtypeStruct((2, rows, cols), jnp.float32)
    return pl.pallas_call(
        functools.partial(subcycle_kernel, rows, cols),
        out_shape=(jax.ShapeDtypeStruct((rows, cols), jnp.float32), pair, pair),
        scratch_shapes=[pltpu.VMEM((3,) + shape, jnp.float32)] * 2,
        cost_estimate=pl.CostEstimate(
            flops=SUB * 1000 * shape[0] * shape[1], bytes_accessed=0, transcendentals=0
        ),
        name="subcycles",
    )(padded)


def body(fields, thickness, cutoff, barotropic, land_sea):
    lon_count, lat_count = lax.axis_size("lon"), lax.axis_size("lat")
    lat_index, lon_index = lax.axis_index("lat"), lax.axis_index("lon")
    components, levels, rows, cols = fields.shape
    circle, total_rows = cols * lon_count, rows * lat_count
    cut, ranks, near, send, take = tables(circle, cols)
    n_far = len(ranks)

    pole_rows = cutoff.shape[0] // 2
    row_ids = lat_index * rows + lax.iota(jnp.int32, rows)
    slots = jnp.where(row_ids < pole_rows, row_ids, row_ids - (total_rows - 2 * pole_rows))
    polar = (row_ids < pole_rows) | (row_ids >= total_rows - pole_rows)
    match = slots[:, None] == lax.broadcasted_iota(jnp.int32, (1, 2 * pole_rows), 1)
    cuts = jnp.sum(jnp.where(match, cutoff[None, :], 0), axis=1)
    cut_rows = polar & (2 * cuts < circle)
    odd = jnp.where(cut_rows, 2 * cuts + 1, 0)
    room = (cols // 128 + 1) * 128
    place = lon_index * cols + lax.iota(jnp.int32, room)
    angle = ((odd[:, None] * place[None, :]) % (2 * circle)).astype(jnp.float32) * (
        math.pi / circle
    )
    cos = jnp.where(cut_rows[:, None], jnp.cos(angle), 0.0)
    sin = jnp.where(cut_rows[:, None], jnp.sin(angle), 0.0)[:, :cols]
    diag = jnp.where(cut_rows, odd.astype(jnp.float32) / circle, 1.0)
    cos = jnp.where(lax.iota(jnp.int32, room)[None] < cols, cos, diag[:, None])

    take_rows = 32 if rows % 32 == 0 else rows
    steps = rows // take_rows
    items = 2 * levels * take_rows
    part = components // 2

    def whole(array):
        return pl.BlockSpec(array.shape, lambda f, h: (0,) * array.ndim)

    def field_spec(first):
        return pl.BlockSpec((1, levels, take_rows, cols), lambda f, h: (f + first, 0, h, 0))

    row_spec = pl.BlockSpec((take_rows, cols), lambda f, h: (h, 0))
    wide_spec = pl.BlockSpec((take_rows, room), lambda f, h: (h, 0))
    pair_spec = pl.BlockSpec((1, take_rows, cols), lambda f, h: (f, h, 0))

    def moment_specs(first):
        return [pl.BlockSpec((r, items), lambda f, h: (0, (f + first) * steps + h)) for r in ranks]

    edges, padded = tall_tile(barotropic, land_sea)
    cos, sin, _ = lax.optimization_barrier((cos, sin, edges))
    moments = pl.pallas_call(
        functools.partial(moment_kernel, ranks),
        grid=(components, steps),
        in_specs=[field_spec(0), wide_spec, row_spec, whole(send)],
        out_specs=moment_specs(0),
        out_shape=[
            jax.ShapeDtypeStruct((r, components * steps * items), jnp.float32) for r in ranks
        ],
        cost_estimate=pl.CostEstimate(
            flops=20 * fields.size * 64, bytes_accessed=4 * fields.size, transcendentals=0
        ),
        name="moments",
    )(fields, cos, sin, send)
    far = [shifted(m, "lon", o + 1, True) for o, m in enumerate(moments[:-1])]
    sea_level, opens, flows = barotropic_steps(padded, rows, cols)
    far, opens, flows = lax.optimization_barrier((far, opens, flows))
    far = far + [moments[-1]]

    def apply(kernel, first, specs, args, name):
        return pl.pallas_call(
            functools.partial(kernel, cut, n_far),
            grid=(part, steps),
            in_specs=[field_spec(first), wide_spec, row_spec]
            + [whole(t) for t in near + (take,)]
            + moment_specs(first)
            + specs,
            out_specs=field_spec(0),
            out_shape=jax.ShapeDtypeStruct((part,) + fields.shape[1:], jnp.float32),
            cost_estimate=pl.CostEstimate(
                flops=12 * part * levels * rows * cols * cols,
                bytes_accessed=4 * fields.size,
                transcendentals=0,
            ),
            name=name,
        )(fields, cos, sin, *near, take, *far, *args)

    tracers = apply(tracer_kernel, 0, [], [], "tracers")
    smem = pl.BlockSpec(memory_space=pltpu.SMEM)
    velocity = apply(
        velocity_kernel, part, [smem, pair_spec, pair_spec], [thickness, opens, flows], "velocity"
    )
    return tracers, velocity, sea_level


def solution(mesh):
    return jax.shard_map(
        body,
        mesh=mesh,
        in_specs=(P(None, None, "lat", "lon"), P(), P(), P(None, "lat", "lon"), P("lat", "lon")),
        out_specs=(P(None, None, "lat", "lon"), P(None, None, "lat", "lon"), P("lat", "lon")),
        check_vma=False,
    )
```

```python
import functools
import math

import jax
import jax.numpy as jnp
import numpy as np
from jax import lax
from jax.experimental import pallas as pl
from jax.experimental.pallas import tpu as pltpu
from jax.sharding import PartitionSpec as P

SUB = 20
HALO = -(-(SUB + 2) // 8) * 8
wave_coef = 0.65
RESIDUAL = 3e-8


def two_part(table):
    high = table.astype(jnp.bfloat16)
    low = (table - high.astype(np.float64)).astype(jnp.bfloat16)
    return high, low


def cosecant(circle, cols, shift):
    gap = (np.arange(cols)[None, :] + shift - np.arange(cols)[:, None]).astype(np.float64)
    sine = np.sin(np.pi * gap / circle)
    near = gap == 0
    return np.where(near, 0.0, 1.0 / np.where(near, 1.0, sine)) / circle


def cross_factors(block):
    rest = block.copy()
    left, right = [], []
    while True:
        spot = np.unravel_index(np.argmax(np.abs(rest)), rest.shape)
        pivot = rest[spot]
        if abs(pivot) < RESIDUAL:
            break
        column = rest[:, spot[1]] / math.sqrt(abs(pivot))
        row = rest[spot[0]] * (math.copysign(1.0, pivot) / math.sqrt(abs(pivot)))
        left.append(column)
        right.append(row)
        rest = rest - column[:, None] * row[None, :]
    pad = -len(left) % 8
    rows, cols = block.shape
    return np.stack(left + [np.zeros(rows)] * pad), np.stack(right + [np.zeros(cols)] * pad)


@functools.lru_cache(maxsize=None)
def tables(circle, cols):
    devices = circle // cols
    cut = -(-cols // 512) * 256
    near = cosecant(circle, cols, 0)
    pairs = [cross_factors(cosecant(circle, cols, cols * o)) for o in range(1, devices)]
    for source, target in ((slice(0, cut), slice(cut, cols)), (slice(cut, cols), slice(0, cut))):
        part = cross_factors(near[source, target])
        whole = [np.zeros((part[0].shape[0], cols)) for _ in range(2)]
        whole[0][:, source], whole[1][:, target] = part
        pairs.append(tuple(whole))
    ranks = tuple(p[0].shape[0] for p in pairs)
    ranks = ranks[: devices - 1] + (sum(ranks[devices - 1 :]),)
    send = two_part(np.concatenate([p[0] for p in pairs]).T)
    width = -(-sum(ranks) // 128) * 128
    room = ((0, 0), (0, width - sum(ranks)))
    send = np.concatenate([np.pad(part, room) for part in send], axis=1)
    take = two_part(np.concatenate([p[1] for p in pairs]))
    take = np.concatenate([take[0], take[0], take[1]])
    side = max(cut, cols - cut)
    return cut, ranks, two_part(near[:side, :side]), send, take


def split(value):
    high = value.astype(jnp.bfloat16)
    low = (value - high.astype(jnp.float32)).astype(jnp.bfloat16)
    return high, low


def dot(a, b):
    return lax.dot_general(a, b, (((1,), (0,)), ((), ())), preferred_element_type=jnp.float32)


def turned(x, cos, sin):
    levels, rows, cols = x.shape
    both = jnp.concatenate([x * cos[None], x * sin[None]], axis=0)
    return split(both.reshape(2 * levels * rows, cols))


def moment_kernel(ranks, x_ref, cos_ref, sin_ref, send_ref, *out_refs):
    cols = x_ref.shape[-1]
    high, low = turned(x_ref[0], cos_ref[:, :cols], sin_ref[:, :cols])
    width = send_ref.shape[1] // 2
    both = dot(high, send_ref[...])
    moments = both[:, :width] + (both[:, width:] + dot(low, send_ref[:, :width]))
    moments = moments.T
    count, place = lax.axis_size("lon"), lax.axis_index("lon")
    start = 0
    for offset, (rank, out_ref) in enumerate(zip(ranks, out_refs), 1):
        group = moments[start : start + rank]
        if offset < count:
            group = group * jnp.where(place + offset >= count, -1.0, 1.0)
        out_ref[...] = group
        start += rank


def filtered_block(cut, n_far, refs):
    x_ref, cos_ref, sin_ref, near_high, near_low, take_ref = refs[:6]
    x = x_ref[0]
    levels, rows, cols = x.shape
    cos, sin = cos_ref[:, :cols], sin_ref[:, :cols]
    diag = cos_ref[:, cols : cols + 1]
    high, low = turned(x, cos, sin)
    far = jnp.concatenate([r[...] for r in refs[6 : 6 + n_far]], axis=0)
    far_high = far.astype(jnp.bfloat16).astype(jnp.float32)
    far = jnp.concatenate([far_high, far - far_high, far_high], axis=0).T.astype(jnp.bfloat16)
    outs = []
    for a, b in ((0, cut), (cut, cols)):
        n = b - a
        k_high, k_low = near_high[:n, :n], near_low[:n, :n]
        part = dot(high[:, a:b], k_high) + (dot(low[:, a:b], k_high) + dot(high[:, a:b], k_low))
        part = (part + dot(far, take_ref[:, a:b])).reshape(2, levels, rows, n)
        outs.append(
            sin[None, :, a:b] * part[0] - cos[None, :, a:b] * part[1] + diag[None] * x[:, :, a:b]
        )
    return outs


def tracer_kernel(cut, n_far, *refs):
    first, second = filtered_block(cut, n_far, refs)
    refs[-1][0, :, :, :cut] = first
    refs[-1][0, :, :, cut:] = second


def velocity_kernel(cut, n_far, *refs):
    thick_ref, open_ref, flow_ref, out_ref = refs[6 + n_far :]
    first, second = filtered_block(cut, n_far, refs)
    cols = out_ref.shape[-1]
    for value, a, b in ((first, 0, cut), (second, cut, cols)):
        column = value[0] * thick_ref[0]
        depth = thick_ref[0]
        for k in range(1, value.shape[0]):
            column = column + value[k] * thick_ref[k]
            depth = depth + thick_ref[k]
        extra = flow_ref[0, :, a:b] - column / jnp.full(column.shape, depth)
        out_ref[0, :, :, a:b] = open_ref[0, :, a:b][None] * (value + extra[None])


def subcycle_kernel(rows, cols, pad_ref, level_ref, open_ref, flow_ref, state, opens):
    high, wide = pad_ref.shape[1:]
    ocean = pad_ref[3]
    opens[0] = ocean * wave_coef
    opens[1] = ocean * pltpu.roll(ocean, wide - 1, 1)
    opens[2] = ocean * pltpu.roll(ocean, high - 1, 0)
    state[0] = pad_ref[0]
    state[1] = pad_ref[1] * opens[1]
    state[2] = pad_ref[2] * opens[2]

    def step(i, carry):
        east, north = state[1], state[2]
        div = east - pltpu.roll(east, 1, 1) + north - pltpu.roll(north, 1, 0)
        surface = state[0] - opens[0] * div
        state[0] = surface
        state[1] = opens[1] * (
            east - wave_coef * (pltpu.roll(surface, wide - 1, 1) - surface)
        )
        state[2] = opens[2] * (
            north - wave_coef * (pltpu.roll(surface, high - 1, 0) - surface)
        )
        return carry

    lax.fori_loop(0, SUB, step, 0)
    level_ref[...] = state[0, :rows, :cols]
    open_ref[...] = opens[1:, :rows, :cols]
    flow_ref[...] = state[1:, :rows, :cols]


def shifted(value, axis, offset, ring):
    count = lax.axis_size(axis)
    pairs = [(i, (i + offset) % count) for i in range(count) if ring or 0 <= i + offset < count]
    return lax.ppermute(value, axis, pairs)


def tall_tile(barotropic, land_sea):
    rows, cols = land_sea.shape
    own = jnp.concatenate([barotropic, land_sea.astype(jnp.float32)[None]])
    west = shifted(own[:, :, cols - HALO :], "lon", 1, True)
    east = shifted(own[:, :, :HALO], "lon", -1, True)
    gap = -(cols + 2 * HALO) % 128
    wide = jnp.concatenate([own, east, jnp.zeros((4, rows, gap), jnp.float32), west], axis=2)
    last, first = wide[:, rows - HALO :], wide[:, :HALO]
    south = shifted(last, "lat", 1, False)
    north = shifted(first, "lat", -1, False)
    return (last, first), jnp.concatenate([wide, north, south], axis=1)


def barotropic_steps(padded, rows, cols):
    shape = padded.shape[1:]
    pair = jax.ShapeDtypeStruct((2, rows, cols), jnp.float32)
    return pl.pallas_call(
        functools.partial(subcycle_kernel, rows, cols),
        out_shape=(jax.ShapeDtypeStruct((rows, cols), jnp.float32), pair, pair),
        scratch_shapes=[pltpu.VMEM((3,) + shape, jnp.float32)] * 2,
        cost_estimate=pl.CostEstimate(
            flops=SUB * 1000 * shape[0] * shape[1], bytes_accessed=0, transcendentals=0
        ),
        name="subcycles",
    )(padded)


def body(fields, thickness, cutoff, barotropic, land_sea):
    lon_count, lat_count = lax.axis_size("lon"), lax.axis_size("lat")
    lat_index, lon_index = lax.axis_index("lat"), lax.axis_index("lon")
    components, levels, rows, cols = fields.shape
    circle, total_rows = cols * lon_count, rows * lat_count
    cut, ranks, near, send, take = tables(circle, cols)
    n_far = len(ranks)

    pole_rows = cutoff.shape[0] // 2
    row_ids = lat_index * rows + lax.iota(jnp.int32, rows)
    slots = jnp.where(row_ids < pole_rows, row_ids, row_ids - (total_rows - 2 * pole_rows))
    polar = (row_ids < pole_rows) | (row_ids >= total_rows - pole_rows)
    match = slots[:, None] == lax.broadcasted_iota(jnp.int32, (1, 2 * pole_rows), 1)
    cuts = jnp.sum(jnp.where(match, cutoff[None, :], 0), axis=1)
    cut_rows = polar & (2 * cuts < circle)
    odd = jnp.where(cut_rows, 2 * cuts + 1, 0)
    room = (cols // 128 + 1) * 128
    place = lon_index * cols + lax.iota(jnp.int32, room)
    angle = ((odd[:, None] * place[None, :]) % (2 * circle)).astype(jnp.float32) * (
        math.pi / circle
    )
    cos = jnp.where(cut_rows[:, None], jnp.cos(angle), 0.0)
    sin = jnp.sin(angle)
    diag = jnp.where(cut_rows, odd.astype(jnp.float32) / circle, 1.0)
    cos = jnp.where(lax.iota(jnp.int32, room)[None] < cols, cos, diag[:, None])

    take_rows = 32 if rows % 32 == 0 else rows
    steps = rows // take_rows
    items = 2 * levels * take_rows
    part = components // 2

    def whole(array):
        return pl.BlockSpec(array.shape, lambda f, h: (0,) * array.ndim)

    def field_spec(first):
        return pl.BlockSpec((1, levels, take_rows, cols), lambda f, h: (f + first, 0, h, 0))

    wide_spec = pl.BlockSpec((take_rows, room), lambda f, h: (h, 0))
    pair_spec = pl.BlockSpec((1, take_rows, cols), lambda f, h: (f, h, 0))

    def moment_specs(first):
        return [pl.BlockSpec((r, items), lambda f, h: (0, (f + first) * steps + h)) for r in ranks]

    edges, padded = tall_tile(barotropic, land_sea)
    cos, sin, _ = lax.optimization_barrier((cos, sin, edges))
    moments = pl.pallas_call(
        functools.partial(moment_kernel, ranks),
        grid=(components, steps),
        in_specs=[field_spec(0), wide_spec, wide_spec, whole(send)],
        out_specs=moment_specs(0),
        out_shape=[
            jax.ShapeDtypeStruct((r, components * steps * items), jnp.float32) for r in ranks
        ],
        cost_estimate=pl.CostEstimate(
            flops=20 * fields.size * 64, bytes_accessed=4 * fields.size, transcendentals=0
        ),
        name="moments",
    )(fields, cos, sin, send)
    far = [shifted(m, "lon", o + 1, True) for o, m in enumerate(moments[:-1])]
    sea_level, opens, flows = barotropic_steps(padded, rows, cols)
    far, opens, flows = lax.optimization_barrier((far, opens, flows))
    far = far + [moments[-1]]

    def apply(kernel, first, specs, args, name):
        return pl.pallas_call(
            functools.partial(kernel, cut, n_far),
            grid=(part, steps),
            in_specs=[field_spec(first), wide_spec, wide_spec]
            + [whole(t) for t in near + (take,)]
            + moment_specs(first)
            + specs,
            out_specs=field_spec(0),
            out_shape=jax.ShapeDtypeStruct((part,) + fields.shape[1:], jnp.float32),
            cost_estimate=pl.CostEstimate(
                flops=12 * part * levels * rows * cols * cols,
                bytes_accessed=4 * fields.size,
                transcendentals=0,
            ),
            name=name,
        )(fields, cos, sin, *near, take, *far, *args)

    tracers = apply(tracer_kernel, 0, [], [], "tracers")
    smem = pl.BlockSpec(memory_space=pltpu.SMEM)
    velocity = apply(
        velocity_kernel, part, [smem, pair_spec, pair_spec], [thickness, opens, flows], "velocity"
    )
    return tracers, velocity, sea_level


def solution(mesh):
    return jax.shard_map(
        body,
        mesh=mesh,
        in_specs=(P(None, None, "lat", "lon"), P(), P(), P(None, "lat", "lon"), P("lat", "lon")),
        out_specs=(P(None, None, "lat", "lon"), P(None, None, "lat", "lon"), P("lat", "lon")),
        check_vma=False,
    )
```
